32 devices in a mesh: row: 8 (over y, x, core), col: 4 (over z).
Axes of the slice: x: 2, y: 2, z: 4, core: 2. Of those that a mesh axis runs over, the one named last changes fastest.
Arguments:
- vectors: bfloat16 [32, 1024, 512], P('col', 'row'), may hold values from -6 to 6
- right_factors: bfloat16 [32, 32, 1024, 128], P('row', 'col'), may hold values from -0.1875 to 0.1875
- left_factors: bfloat16 [32, 32, 1024, 128], P('row', 'col'), may hold values from -0.125 to 0.125
- tile_ranks: int32 [32, 32], P('row', 'col'), may hold values from 16 to 128
- owner_map: int32 [32], replicated, may hold values from 0 to 31, as said below
Outputs:
- applied: bfloat16 [32, 1024, 512], P('row', 'col')
The draws below stay inside these ranges and needn't reach their ends.
Inputs may be any that keep to these rules, and one draw needn't show every extreme that they name: owner_map is a permutation of 0 to 31; the 4 stored tile rows held by index i of row (stored rows i * 4 to i * 4 + 3) belong to 4 different indices of row of applied, i + c mod 8 for the same 4 offsets c at every i.
All inputs are finite; a program needn't handle non-finite values.
Results may differ from the reference program's by a relative error of at most 0.0066.
Values may be sent and summed in bfloat16 or wider, within the bound.
No kernel may reach another device: no remote copies, remote signals or barrier semaphores. Data moves between devices by JAX's collectives and lax.ppermute only.
A program may use at most 128 MiB of HBM per device.

```python
import jax
import jax.numpy as jnp
from jax import lax

BLK = 1024
RMAX = 128
TRD = 4
NV = 512
NT = 32
MT = 32
N_ROW = 8


def shuffle(subkey):
    return jax.random.permutation(subkey, TRD)


def draw_owner_map(key, part):
    key_shift, key_dest, key_source = jax.random.split(jax.random.fold_in(key, 17), 3)
    offsets = jnp.arange(N_ROW, dtype=jnp.int32)
    ranking = jax.random.permutation(key_shift, N_ROW).astype(jnp.int32)
    priority = jnp.where(offsets == N_ROW // 2, -2, jnp.where(offsets == 1, -1, ranking))
    shifts = jnp.argsort(priority)[:TRD].astype(jnp.int32)
    dest_order = jax.vmap(shuffle)(jax.random.split(key_dest, N_ROW)).astype(jnp.int32)
    source_order = jax.vmap(shuffle)(jax.random.split(key_source, N_ROW)).astype(jnp.int32)
    source = jnp.arange(N_ROW, dtype=jnp.int32)[:, None]
    group_index = jnp.broadcast_to(jnp.arange(TRD, dtype=jnp.int32)[None, :], (N_ROW, TRD))
    target = (source + shifts[None, :]) % N_ROW
    landing = target * TRD + dest_order[target, group_index]
    places = source * TRD + source_order
    return jnp.zeros((MT,), jnp.int32).at[places.reshape(-1)].set(landing.reshape(-1))


def with_ends(entries, own_key, low, top_value):
    place = [jax.random.randint(jax.random.fold_in(own_key, axis), (), 0, length) for axis, length in enumerate(entries.shape)]
    main_axis = entries.shape.index(max(entries.shape))
    neighbour = place[:main_axis] + [(place[main_axis] + 1) % entries.shape[main_axis]] + place[main_axis + 1:]
    return entries.at[tuple(place)].set(low).at[tuple(neighbour)].set(top_value)


def block_scale(own_key, extent, cuts, least, largest):
    level, own = 1.0, jax.random.fold_in(own_key, 6)
    for axis_at, shards_of in cuts:
        heights = jnp.exp(jax.random.uniform(jax.random.fold_in(own, axis_at), (shards_of,), jnp.float32, least / len(cuts), largest / len(cuts)))
        level = level * jnp.repeat(heights, extent[axis_at] // shards_of).reshape([-1 if axis == axis_at else 1 for axis in range(len(extent))])
    return level


def centred(key, dims, width, limit, shards=(), kind=jnp.bfloat16):
    values = jax.random.normal(key, dims, jnp.float32) * width
    if len(shards) > 0:
        values = block_scale(key, dims, shards, -0.22, 0.18) * values
    return jnp.clip(values, min=-limit, max=limit).astype(kind)


def setup_inputs(seed: int = 0) -> dict:
    keys = jax.random.split(jax.random.key(seed), 6)
    return {
        "vectors": centred(keys[0], (NT, BLK, NV), 1.0, 6.0, ((0, 4), (1, 8))),
        "right_factors": centred(keys[1], (MT, NT, BLK, RMAX), BLK ** -0.5, 0.1875, ((0, 8), (1, 4))),
        "left_factors": centred(keys[2], (MT, NT, BLK, RMAX), (NT * RMAX // 2) ** -0.5, 0.125, ((0, 8), (1, 4))),
        "tile_ranks": with_ends(jax.random.randint(keys[3], (MT, NT), RMAX // 8, RMAX + 1), jax.random.fold_in(keys[3], 1), RMAX // 8, RMAX).astype(jnp.int32),
        "owner_map": draw_owner_map(jax.random.fold_in(keys[5], 71), 0),
    }


def reference(vectors, right_factors, left_factors, tile_ranks, owner_map):
    columns = jnp.arange(RMAX, dtype=jnp.int32)
    wide_vectors = vectors.astype(jnp.float32)

    def tile_row(operands):
        left_row, right_row, rank_row = operands
        products = jnp.einsum("kbr,kbv->krv", right_row.astype(jnp.float32), wide_vectors)
        kept_mask = columns[None, :] < rank_row[:, None]
        coeffs = jnp.where(kept_mask[:, :, None], products, 0.0).astype(jnp.bfloat16)
        return jnp.einsum("kbr,krv->bv", left_row.astype(jnp.float32), coeffs.astype(jnp.float32))

    stored = lax.map(tile_row, (left_factors, right_factors, tile_ranks))
    natural = jnp.zeros(stored.shape, jnp.float32).at[owner_map].set(stored)
    return natural.astype(jnp.bfloat16)
```

```python
import jax
import jax.numpy as jnp
from jax import lax
from jax.sharding import PartitionSpec as P

CHUNKS = (1, 1)
TIE = True
GATHER = "perm"
SCATTER = "xla"


def masked_coeffs(products, tile_ranks, rank_width):
    columns = jnp.arange(rank_width, dtype=jnp.int32)
    kept_mask = columns[None, None, :] < tile_ranks[:, :, None]
    return jnp.where(kept_mask[:, :, :, None], products, 0.0).astype(jnp.bfloat16)


def build_buffer(payload, owner_map, cycle_size):
    held_rows = payload.shape[0]
    own_rows = lax.dynamic_slice_in_dim(owner_map, lax.axis_index("row") * held_rows, held_rows)
    target = own_rows // held_rows
    devices = jnp.arange(cycle_size, dtype=jnp.int32)
    matches = target[None, :] == devices[:, None]
    source_slot = jnp.sum(
        jnp.where(matches, jnp.arange(held_rows, dtype=jnp.int32)[None, :], 0), axis=1
    )
    return jnp.take(payload, source_slot, axis=0)


def pick_rows(received, owner_map, held_rows):
    wanted = lax.axis_index("row") * held_rows + jnp.arange(held_rows, dtype=jnp.int32)
    matches = owner_map[None, :] == wanted[:, None]
    anchor = jnp.sum(
        jnp.where(matches, jnp.arange(owner_map.shape[0], dtype=jnp.int32)[None, :], 0), axis=1
    )
    return jnp.take(received, anchor // held_rows, axis=0)


def flip(x, bit, size):
    return lax.ppermute(x, "row", [(i, i ^ bit) for i in range(size)])


def gather_rows(block, gate):
    size = lax.axis_size("row")
    tiles, rows, width = block.shape
    if GATHER == "xla" or size & (size - 1) or tiles % 2:
        return lax.all_gather(block, "row", axis=1, tiled=True), []
    half = tiles // 2
    bits = [1 << b for b in range(1, size.bit_length() - 1)]
    held = {0: [(0, block)]}
    gated = False
    for m in sorted(range(2, size, 2), key=lambda m: (bin(m).count("1"), m)):
        on = [b for b in bits if m & b]
        if len(on) == 1:
            held[m] = [(0, flip(held[0][0][1], on[0], size))]
        else:
            if gate is not None and not gated:
                firsts = [held[b][0][1] for b in bits]
                block, firsts, _ = lax.optimization_barrier((block, firsts, gate))
                held[0] = [(0, block)]
                for b, piece in zip(bits, firsts):
                    held[b] = [(0, piece)]
                gated = True
            pieces = []
            for start, bit in ((0, on[-1]), (half, on[0])):
                for at, piece in held[m ^ bit]:
                    if piece.shape[0] == tiles:
                        pieces.append((start, flip(piece[start:start + half], bit, size)))
                    elif at == start:
                        pieces.append((start, flip(piece, bit, size)))
            held[m] = pieces
    for m in range(0, size, 2):
        held[m + 1] = [(at, flip(piece, 1, size)) for at, piece in held[m]]
    arrived = [piece for m in sorted(held) if m for _, piece in held[m]]
    me = lax.axis_index("row")
    whole = jnp.zeros((tiles, size, rows, width), block.dtype)
    for m in sorted(held):
        for at, piece in held[m]:
            whole = lax.dynamic_update_slice(whole, piece[:, None], (at, me ^ m, 0, 0))
    return whole.reshape(tiles, size * rows, width), arrived


def scatter_rows(partial):
    size = lax.axis_size("col")
    held_rows, rows, width = partial.shape
    if SCATTER == "xla":
        return lax.psum_scatter(partial, "col", scatter_dimension=1, tiled=True)
    me = lax.axis_index("col")
    share = rows // size

    def part(index):
        at = jnp.clip(index, 0, size - 1) * share
        return lax.dynamic_slice(partial, (0, at, 0), (held_rows, share, width))

    up, down = None, None
    for t in range(1, size):
        pairs = [(i, i + 1) for i in range(t)]
        back = [(size - 1 - i, size - 1 - j) for i, j in pairs]
        send_up, send_down = part(size - t + me), part(t - size + me)
        if up is not None:
            send_up = (send_up.astype(jnp.float32) + up.astype(jnp.float32)).astype(jnp.bfloat16)
            send_down = (send_down.astype(jnp.float32) + down.astype(jnp.float32)).astype(jnp.bfloat16)
        up = lax.ppermute(send_up, "col", pairs)
        down = lax.ppermute(send_down, "col", back)
    total = part(me).astype(jnp.float32)
    if up is not None:
        total = total + up.astype(jnp.float32) + down.astype(jnp.float32)
    return total.astype(jnp.bfloat16)


def on_device(vectors, right_factors, left_factors, tile_ranks, owner_map):
    held_rows = right_factors.shape[0]
    rank_width = right_factors.shape[3]
    cycle_size = lax.axis_size("row")
    unit = vectors.shape[2] // sum(CHUNKS)
    parts = []
    hops = []
    at = 0
    partial_rows = None
    for portion in CHUNKS:
        block = vectors[:, :, at:at + portion * unit]
        at += portion * unit
        if TIE and hops:
            block, _ = lax.optimization_barrier((block, hops))
        gathered, hops = gather_rows(block, partial_rows if TIE else None)
        products = jnp.einsum(
            "ikbr,kbv->ikrv",
            right_factors,
            gathered,
            preferred_element_type=jnp.float32,
        )
        coeffs = masked_coeffs(products, tile_ranks, rank_width)
        partial_rows = jnp.einsum(
            "ikbr,ikrv->ibv", left_factors, coeffs, preferred_element_type=jnp.float32
        ).astype(jnp.bfloat16)
        summed = scatter_rows(partial_rows)
        if parts:
            summed, received = lax.optimization_barrier((summed, received))
            parts[-1] = pick_rows(received, owner_map, held_rows)
        buffer = build_buffer(summed, owner_map, cycle_size)
        received = lax.all_to_all(buffer, "row", split_axis=0, concat_axis=0, tiled=True)
        parts.append(pick_rows(received, owner_map, held_rows))
    return jnp.concatenate(parts, axis=2)


def solution(mesh):
    placed = (
        P("col", "row", None),
        P("row", "col", None, None),
        P("row", "col", None, None),
        P("row", "col"),
        P(),
    )
    return jax.shard_map(
        on_device, mesh=mesh, in_specs=placed, out_specs=P("row", "col", None), check_vma=False
    )
```
